32 devices in a mesh: seq: 2 (over core), batch: 16 (over z, y, x).
Axes of the slice: x: 2, y: 2, z: 4, core: 2. Of those that a mesh axis runs over, the one named last changes fastest.
Arguments:
- queries: bfloat16 [16, 1024, 1024], P('batch', 'seq'), may hold values from -6 to 6
- keys: bfloat16 [16, 1024, 1024], P('batch', 'seq'), may hold values from -6 to 6
- values: bfloat16 [16, 1024, 2048], P('batch', 'seq'), may hold values from -6 to 6
- gate_rate: bfloat16 [16, 1024, 1024], P('batch', 'seq'), may hold values from 0.5 to 2
- segment_ids: int32 [16, 1024], P('batch', 'seq'), may hold values from 0 to 2, never falling along the last dimension, each value on 1 to 512 neighbouring positions
- decay_exps: int32 [4], replicated, may hold values from 0 to 13
- out_weight: bfloat16 [2048, 2048], P('batch'), may hold values from -0.125 to 0.125
Outputs:
- projected: bfloat16 [16, 1024, 2048], P('batch', 'seq')
The draws below stay inside these ranges and needn't reach their ends.
Inputs may be any that keep to these rules, and one draw needn't show every extreme that they name: `segment_ids`: within each stream the ids never fall and start at 0; each of the 3 ids covers 1 to 512 consecutive tokens, one of them exactly 512.
All inputs are finite; a program needn't handle non-finite values.
Results may differ from the reference program's by a relative error of at most 0.004.
The reference program's roundings to bfloat16 on the way (of `hidden`) count: a program that leaves them out, or rounds other values in their place, can miss the bound.
Values may be sent and summed in bfloat16 or wider, within the bound.
A program may use at most 128 MiB of HBM per device.

```python
import math
import jax
import jax.numpy as jnp
import numpy as np
from jax import lax

D = 2048
HEADS = 4
HEAD_K = 256
BLOCK = 64
SEGS = 3
SEQLEN = 1024
GROUPS = 16
KEYS = 1024
VALS = 2048


def place_ends(values, own_key, low, top_value):
    longest = values.shape.index(max(values.shape))
    spots = []
    for shift in (0, 1):
        where = [jax.random.randint(jax.random.fold_in(own_key, axis), (), 0, length) for axis, length in enumerate(values.shape)]
        where[longest] = (where[longest] + shift) % values.shape[longest]
        spots.append(tuple(where))
    return values.at[spots[0]].set(low).at[spots[1]].set(top_value)


def steps_of(rng, extent, cuts, low, top_value):
    def one(position, blocks):
        draws = jax.random.uniform(jax.random.fold_in(jax.random.fold_in(rng, 6), position), (blocks,), jnp.float32, low / len(cuts), top_value / len(cuts))
        return jnp.repeat(jnp.exp(draws), extent[position] // blocks).reshape((-1,) + (1,) * (len(extent) - position - 1))

    level = one(*cuts[0])
    for cut in cuts[1:]:
        level = level * one(*cut)
    return level


def profile(count, total, reach, skew):
    portions = [(1 << 20) // math.isqrt(standing ** skew) + 1 for standing in range(2, count + 1)]
    surplus, holding = total - reach - (count - 1), [1] * (count - 1)
    while surplus > 0:
        movable = [i for i in range(count - 1) if holding[i] < reach]
        pool, remaining = sum([portions[i] for i in movable]), surplus
        for i in movable:
            extra = min(reach - holding[i], max(1, remaining * portions[i] // pool), surplus)
            holding[i] = holding[i] + extra
            surplus = surplus - extra
    return np.array([reach] + holding)


def ragged(own_key, number_of, total, most, skew):
    if number_of == 2:
        one = jax.random.randint(own_key, (), max(1, total - most), min(most, total - 1) + 1)
        return jnp.stack([one, total - one])
    sizes = jnp.asarray(profile(number_of, total, most, skew), jnp.int32)
    pairs = (number_of - 1) // 2
    giver, taker = sizes[1:1 + 2 * pairs:2], sizes[2:2 + 2 * pairs:2]
    margin = jnp.minimum(giver - 1, most - taker)
    shifted = jax.random.randint(jax.random.fold_in(own_key, 1), (pairs,), 0, 1 << 20) % (margin + 1)
    sizes = sizes.at[1:1 + 2 * pairs:2].set(giver - shifted).at[2:2 + 2 * pairs:2].set(taker + shifted)
    return sizes[jax.random.permutation(jax.random.fold_in(own_key, 2), number_of)]


def centred(stream_key, shape, scale, limit, cuts=(), kind=jnp.bfloat16):
    values = jax.random.normal(stream_key, shape, jnp.float32) * scale
    if len(cuts) > 0:
        values = steps_of(stream_key, shape, cuts, -0.22, 0.18) * values
    return jnp.clip(values, min=-limit, max=limit).astype(kind)


def setup_inputs(seed: int = 0) -> dict:
    arg_keys = jax.random.split(jax.random.key(seed), 8)
    return {
        "queries": centred(arg_keys[0], (GROUPS, SEQLEN, KEYS), 1.0, 6.0, ((0, 16), (1, 2))),
        "keys": centred(arg_keys[1], (GROUPS, SEQLEN, KEYS), 1.0, 6.0, ((0, 16), (1, 2))),
        "values": centred(arg_keys[2], (GROUPS, SEQLEN, VALS), 1.0, 6.0, ((0, 16), (1, 2))),
        "gate_rate": jnp.clip(jnp.exp(math.log(2.0) - 1.3862944 * jax.random.uniform(arg_keys[3], (GROUPS, SEQLEN, KEYS), jnp.float32) ** steps_of(arg_keys[3], (GROUPS, SEQLEN, KEYS), ((0, 16), (1, 2)), -0.2, 0.2)), 0.5, 2.0).astype(jnp.bfloat16),
        "segment_ids": jax.vmap(lambda own: jnp.searchsorted(jnp.cumsum(ragged(own, SEGS, SEQLEN, SEQLEN // 2, 2)), jnp.arange(SEQLEN), side="right"))(jax.random.split(arg_keys[4], GROUPS)).reshape((GROUPS, SEQLEN)).astype(jnp.int32),
        "decay_exps": place_ends(jax.random.randint(arg_keys[5], (HEADS,), 0, 14), jax.random.fold_in(arg_keys[5], 1), 0, 13).astype(jnp.int32),
        "out_weight": centred(arg_keys[6], (VALS, D), VALS ** -0.5, 0.125, ((0, 16),)),
    }


def linear_blocks(lifted_query, key_heads, value_heads, log_decay, starts, initial):
    groups, length, head_count, key_width = lifted_query.shape
    value_width = value_heads.shape[3]
    block_count = length // BLOCK

    def split(member):
        return jnp.swapaxes(member.reshape((groups, block_count, BLOCK) + member.shape[2:]), 0, 1)

    def advance(carried, pieces):
        query_rows, key_rows, value_rows, log_rows, start_rows = pieces
        running = jnp.cumsum(log_rows, axis=1)
        segment_rank = jnp.cumsum(start_rows, axis=1)
        unbroken = (segment_rank == 0).astype(jnp.float32)
        raised_q = query_rows * jnp.exp(running)
        raised_k = key_rows * jnp.exp(-running)
        scores = jnp.einsum('gthc,gshc->ghts', raised_q, raised_k, precision=lax.Precision.HIGHEST)
        order = jnp.arange(BLOCK)
        causal = order[:, None] >= order[None, :]
        same_doc = segment_rank[:, :, None] == segment_rank[:, None, :]
        allowed = jnp.logical_and(causal[None], same_doc).astype(jnp.float32)
        inside = jnp.einsum('ghts,gshv->gthv', scores * allowed[:, None], value_rows, precision=lax.Precision.HIGHEST)
        outside = unbroken[:, :, None, None] * jnp.einsum('gthc,ghcv->gthv', raised_q, carried, precision=lax.Precision.HIGHEST)
        final_log = running[:, -1]
        in_last = (segment_rank == segment_rank[:, -1:]).astype(jnp.float32)
        weighted = key_rows * jnp.exp(final_log[:, None] - running) * in_last[:, :, None, None]
        kept = unbroken[:, -1][:, None, None, None] * jnp.exp(final_log)[..., None] * carried
        updated = kept + jnp.einsum('gshc,gshv->ghcv', weighted, value_rows, precision=lax.Precision.HIGHEST)
        return (updated, inside + outside)
    members = (lifted_query, key_heads, value_heads, log_decay, starts)
    final, outputs = lax.scan(advance, initial, tuple((split(member) for member in members)))
    outputs = jnp.swapaxes(outputs, 0, 1).reshape(groups, length, head_count, value_width)
    return (outputs, final)

def reference(queries, keys, values, gate_rate, segment_ids, decay_exps, out_weight):
    groups = queries.shape[0]
    length = queries.shape[1]
    head_count = decay_exps.shape[0]

    def heads_of(array):
        return array.astype(jnp.float32).reshape(groups, length, head_count, -1)
    scaling = jnp.exp2(-decay_exps.astype(jnp.float32)) / 16.0
    log_decay = -heads_of(gate_rate) * scaling[None, None, :, None]
    previous = jnp.concatenate([jnp.full((groups, 1), -1, jnp.int32), segment_ids[:, :-1]], axis=1)
    starts = (segment_ids != previous).astype(jnp.float32)
    query_heads = heads_of(queries) * (1.0 / math.sqrt(HEAD_K))
    key_heads = heads_of(keys)
    value_heads = heads_of(values)
    initial = jnp.zeros((groups, head_count, key_heads.shape[3], value_heads.shape[3]), jnp.float32)
    mixed, final = linear_blocks(query_heads, key_heads, value_heads, log_decay, starts, initial)
    normed = mixed / jnp.sqrt(lax.optimization_barrier(jnp.mean(mixed * mixed, axis=-1, keepdims=True)) + 1.0)
    hidden = normed.astype(jnp.bfloat16).reshape(groups * length, -1)
    product = jnp.dot(hidden, out_weight, preferred_element_type=jnp.float32)
    return product.astype(jnp.bfloat16).reshape(groups, length, -1)
```

```python
import functools
import math

import jax
import jax.numpy as jnp
from jax import lax
from jax.experimental import pallas as pl
from jax.experimental.pallas import tpu as pltpu
from jax.sharding import PartitionSpec as P

MESH = pl.DeviceIdType.MESH
CHUNK = 256
TILE = 512


def chip_grid(mesh):
    count = mesh.shape["batch"]
    try:
        axis = mesh.axis_names.index("batch")
        line = mesh.devices.swapaxes(0, axis).reshape(count, -1)[:, 0]
        coords = [tuple(device.coords) for device in line]
        sizes = [len({c[i] for c in coords}) for i in (2, 1, 0)]
        lows = [min(c[i] for c in coords) for i in (2, 1, 0)]
        for index, c in enumerate(coords):
            z, y, x = (c[2] - lows[0], c[1] - lows[1], c[0] - lows[2])
            if (z * sizes[1] + y) * sizes[2] + x != index:
                return (count, 1, 1)
        return tuple(sizes)
    except Exception:
        return (count, 1, 1)


def split(x):
    high = x.astype(jnp.bfloat16)
    return high, (x - high.astype(jnp.float32)).astype(jnp.bfloat16)


def mm(a, b):
    return lax.dot_general(a, b, (((1,), (0,)), ((), ())), preferred_element_type=jnp.float32)


def mm_t(a, b):
    return lax.dot_general(a, b, (((1,), (1,)), ((), ())), preferred_element_type=jnp.float32)


def t_mm(a, b):
    return lax.dot_general(a, b, (((0,), (0,)), ((), ())), preferred_element_type=jnp.float32)


def kernel(
    grid, peers, heads, chunk,
    q_hbm, k_hbm, v_hbm, g_hbm, seg_ref, exps_ref, w_hbm,
    out_hbm,
    q_ref, k_ref, v_ref, g_ref, w_ref, hidden, acc, out_ref, seg_in, state_in, state_out,
    load_sem, out_sem, seg_sem, state_send, state_recv, send_sem, recv_sem, msend, mrecv,
):
    Z, Y, X = grid
    s = lax.axis_index("seq")
    me = lax.axis_index("batch")
    length, keys = q_ref.shape
    key_width = keys // heads
    value_width = v_ref.shape[1] // heads
    rows = w_hbm.shape[0]
    columns = w_ref.shape[1]
    part = columns // peers
    plane_rows = rows * X * Y
    a = me // (X * Y)
    swap = X == Y
    nb, nc = X, Y

    def strides(core):
        if not swap:
            return 1, X
        even = lax.rem(core, 2) == 0
        return jnp.where(even, 1, X), jnp.where(even, X, 1)

    def chip_back(core, da, db, dc):
        sb, sc = strides(core)
        b = lax.rem(me // sb, nb)
        c = lax.rem(me // sc, nc)
        return (
            lax.rem(a - da + Z, Z) * (X * Y)
            + lax.rem(b - db + nb, nb) * sb
            + lax.rem(c - dc + nc, nc) * sc
        )

    def label(da, db, dc):
        return (da * nb + db) * nc + dc

    def block(core, chip):
        return w_ref.at[
            pl.ds(pl.multiple_of(chip * rows, rows), rows),
            pl.ds(pl.multiple_of(core * part, part), part),
        ]

    def relay(held, step):
        da, db, dc = (h + t for h, t in zip(held, step))
        here = block(s, chip_back(s, *held))
        target = chip_back(s, -step[0], -step[1], -step[2])
        index = label(da, db, dc)
        return pltpu.make_async_remote_copy(
            src_ref=here, dst_ref=here, send_sem=send_sem.at[index], recv_sem=recv_sem.at[index],
            device_id={"batch": target}, device_id_type=MESH,
        )

    def arrival(da, db, dc):
        here = block(s, chip_back(s, da, db, dc))
        index = label(da, db, dc)
        other = lax.rem(me + 1, X * Y * Z)
        return pltpu.make_async_remote_copy(
            src_ref=here, dst_ref=here, send_sem=send_sem.at[index], recv_sem=recv_sem.at[index],
            device_id={"batch": other}, device_id_type=MESH,
        )

    def mirror(da, db, dc, ds, core):
        here = block(core, chip_back(core, da, db, dc))
        index = label(da, db, dc)
        return pltpu.make_async_remote_copy(
            src_ref=here, dst_ref=here,
            send_sem=msend.at[ds - 1, index], recv_sem=mrecv.at[ds - 1, index],
            device_id={"seq": lax.rem(s + ds, peers)}, device_id_type=MESH,
        )

    def share(da, db, dc):
        for ds in range(1, peers):
            mirror(da, db, dc, ds, s).start()

    def forward_plane(g):
        for db in range(1, nb):
            relay((g, 0, 0), (0, db, 0)).start()
        for dc in range(1, nc):
            relay((g, 0, 0), (0, 0, dc)).start()

    def middle(g):
        for db in range(1, nb):
            arrival(g, db, 0).wait_recv()
            for dc in range(1, nc):
                relay((g, db, 0), (0, 0, dc)).start()
            share(g, db, 0)

    def enter(g):
        @pl.when(g < Z)
        def _():
            arrival(g, 0, 0).wait_recv()
            forward_plane(g)
            share(g, 0, 0)

    def tail(g):
        for dc in range(1, nc):
            for db in range(nb):
                arrival(g, db, dc).wait_recv()
                share(g, db, dc)

    def mirrored(g):
        for ds in range(1, peers):
            core = lax.rem(s - ds + peers, peers)
            for db in range(nb):
                for dc in range(nc):
                    def wait():
                        mirror(g, db, dc, ds, core).wait_recv()
                    if db or dc:
                        wait()
                    else:
                        pl.when(g > 0)(wait)

    loads = [
        pltpu.make_async_copy(
            w_hbm, w_ref.at[pl.ds(pl.multiple_of(me * rows, rows), rows), :], load_sem.at[0]
        ),
        pltpu.make_async_copy(g_hbm, g_ref, load_sem.at[1]),
        pltpu.make_async_copy(k_hbm, k_ref, load_sem.at[2]),
        pltpu.make_async_copy(q_hbm, q_ref, load_sem.at[3]),
        pltpu.make_async_copy(v_hbm, v_ref, load_sem.at[4]),
    ]
    for load in loads:
        load.start()

    barrier = pltpu.get_barrier_semaphore()
    friends = [{"batch": chip_back(s, d, 0, 0)} for d in range(1, Z)]
    friends += [{"batch": chip_back(s, 0, d, 0)} for d in range(1, nb)]
    friends += [{"batch": chip_back(s, 0, 0, d)} for d in range(1, nc)]
    friends += [{"seq": lax.rem(s + d, peers)} for d in range(1, peers)]
    for friend in friends:
        pl.semaphore_signal(barrier, inc=1, device_id=friend, device_id_type=MESH)
    pl.semaphore_wait(barrier, len(friends))

    loads[0].wait()
    for da in range(1, Z):
        relay((0, 0, 0), (da, 0, 0)).start()
    forward_plane(0)

    def next_core():
        return {"seq": lax.rem(s + 1, peers)}

    seg_copy = pltpu.make_async_remote_copy(
        src_ref=seg_ref, dst_ref=seg_in, send_sem=seg_sem.at[0], recv_sem=seg_sem.at[1],
        device_id=next_core(), device_id_type=MESH,
    )

    def state_copy(h):
        return pltpu.make_async_remote_copy(
            src_ref=state_out.at[h], dst_ref=state_in.at[h],
            send_sem=state_send.at[h], recv_sem=state_recv.at[h],
            device_id=next_core(), device_id_type=MESH,
        )

    @pl.when(s < peers - 1)
    def _():
        seg_copy.start()

    @pl.when(s == 0)
    def _():
        state_in[...] = jnp.zeros_like(state_in)
        seg_in[...] = jnp.full(seg_in.shape, -1, jnp.int32)

    for load in loads[1:]:
        load.wait()

    @pl.when(s > 0)
    def _():
        seg_copy.wait_recv()

    order_t = lax.broadcasted_iota(jnp.int32, (chunk, chunk), 0)
    order_s = lax.broadcasted_iota(jnp.int32, (chunk, chunk), 1)
    causal = order_t >= order_s
    triangle = jnp.where(causal, 1.0, 0.0).astype(jnp.bfloat16)
    seg_row = seg_ref[...].astype(jnp.float32)
    before = seg_in[...].astype(jnp.float32)[:, length - 1:]
    seg_wide = jnp.broadcast_to(seg_row, (128, length)).T

    def head(h, _):
        exponent = jnp.full((1, key_width), exps_ref[h], jnp.int32).astype(jnp.float32)
        scale = jnp.exp2(-exponent) * (-1.0 / 16.0)

        @pl.when(s > 0)
        def _():
            state_copy(h).wait_recv()

        state = state_in[h]
        previous = before
        key_cols = pl.ds(pl.multiple_of(h * key_width, key_width), key_width)
        value_cols = pl.ds(pl.multiple_of(h * value_width, value_width), value_width)
        for i in range(length // chunk):
            now = pl.ds(i * chunk, chunk)
            log = mm(triangle, g_ref[now, key_cols]) * scale
            fall = jnp.exp(log)
            raised_q = q_ref[now, key_cols].astype(jnp.float32) * (fall * (1.0 / math.sqrt(key_width)))
            raised_k = k_ref[now, key_cols].astype(jnp.float32) * jnp.exp(-log)
            value = v_ref[now, value_cols]
            q_hi, q_lo = split(raised_q)
            k_hi, k_lo = split(raised_k)
            row = seg_row[:, i * chunk:(i + 1) * chunk]
            column = seg_wide[i * chunk:(i + 1) * chunk, :1]
            scores = mm_t(q_hi, k_hi) + mm_t(q_hi, k_lo) + mm_t(q_lo, k_hi)
            scores = jnp.where(jnp.logical_and(causal, column == row), scores, 0.0)
            p_hi, p_lo = split(scores)
            s_hi, s_lo = split(state)
            carried = mm_t(q_hi, s_hi) + mm_t(q_hi, s_lo) + mm_t(q_lo, s_hi)
            mixed = mm(p_hi, value) + mm(p_lo, value)
            mixed = mixed + jnp.where(column == previous, carried, 0.0)
            power = jnp.mean(mixed * mixed, axis=-1, keepdims=True)
            hidden[now, value_cols] = (mixed * lax.rsqrt(power + 1.0)).astype(jnp.bfloat16)
            final = fall[chunk - 1:, :]
            last = row[:, chunk - 1:]
            weighted = jnp.where(column == last, raised_k * final, 0.0)
            w_hi, w_lo = split(weighted)
            kept = jnp.where(last == previous, state * final, 0.0)
            state = kept + t_mm(value, w_hi) + t_mm(value, w_lo)
            previous = last

        @pl.when(s < peers - 1)
        def _():
            state_out[h] = state
            state_copy(h).start()

        @pl.when(h == (heads - 1) // 2)
        def _():
            middle(0)
            enter(1)

        return 0

    lax.fori_loop(0, heads, head, 0)

    def plane_start(g):
        return pl.multiple_of(lax.rem(a - g + Z, Z) * plane_rows, plane_rows)

    def project(g):
        start = plane_start(g)
        left = hidden[:, pl.ds(start, plane_rows)]
        for tile in range(columns // TILE):
            cols = pl.ds(tile * TILE, TILE)
            product = mm(left, w_ref[pl.ds(start, plane_rows), cols])

            @pl.when(g == 0)
            def _():
                acc[:, cols] = product

            @pl.when(g > 0)
            def _():
                acc[:, cols] += product

    def step(g, _):
        middle(g)
        enter(g + 1)
        tail(g - 1)
        mirrored(g - 1)
        project(g - 1)
        return 0

    lax.fori_loop(1, Z, step, 0)
    tail(Z - 1)
    mirrored(Z - 1)
    start = plane_start(Z - 1)
    left = hidden[:, pl.ds(start, plane_rows)]
    stores = []
    for tile in range(columns // TILE):
        cols = pl.ds(tile * TILE, TILE)
        product = mm(left, w_ref[pl.ds(start, plane_rows), cols])
        total = acc[:, cols] + product if Z > 1 else product
        out_ref[:, cols] = total.astype(jnp.bfloat16)
        store = pltpu.make_async_copy(out_ref.at[:, cols], out_hbm.at[:, cols], out_sem.at[tile])
        store.start()
        stores.append(store)

    @pl.when(s < peers - 1)
    def _():
        seg_copy.wait_send()

        def sent(h, _):
            state_copy(h).wait_send()
            return 0

        lax.fori_loop(0, heads, sent, 0)

    def sent_block(index, _):
        da, rest = index // (nb * nc), lax.rem(index, nb * nc)
        db, dc = rest // nc, lax.rem(rest, nc)
        arrival(da, db, dc).wait_send()
        for ds in range(1, peers):
            mirror(da, db, dc, ds, s).wait_send()
        return 0

    lax.fori_loop(1, Z * nb * nc, sent_block, 0)
    for store in stores:
        store.wait()


def local(grid, peers, queries, keys, values, gate_rate, segment_ids, decay_exps, out_weight):
    groups, length, key_features = queries.shape
    heads = decay_exps.shape[0]
    features = values.shape[2]
    columns = out_weight.shape[1]
    chips = grid[0] * grid[1] * grid[2]
    chunk = min(CHUNK, length)
    kw, vw = key_features // heads, features // heads
    bf16, f32 = jnp.bfloat16, jnp.float32
    anywhere = pl.BlockSpec(memory_space=pl.ANY)
    call = pl.pallas_call(
        functools.partial(kernel, grid, peers, heads, chunk),
        out_shape=jax.ShapeDtypeStruct((length, columns), bf16),
        in_specs=[anywhere] * 4
        + [pl.BlockSpec(memory_space=pltpu.VMEM), pl.BlockSpec(memory_space=pltpu.SMEM), anywhere],
        out_specs=anywhere,
        scratch_shapes=[
            pltpu.VMEM((length, key_features), bf16),
            pltpu.VMEM((length, key_features), bf16),
            pltpu.VMEM((length, features), bf16),
            pltpu.VMEM((length, key_features), bf16),
            pltpu.VMEM((features, columns), bf16),
            pltpu.VMEM((length, features), bf16),
            pltpu.VMEM((length, columns), f32),
            pltpu.VMEM((length, columns), bf16),
            pltpu.VMEM((1, length), jnp.int32),
            pltpu.VMEM((heads, vw, kw), f32),
            pltpu.VMEM((heads, vw, kw), f32),
            pltpu.SemaphoreType.DMA((5,)),
            pltpu.SemaphoreType.DMA((columns // TILE,)),
            pltpu.SemaphoreType.DMA((2,)),
            pltpu.SemaphoreType.DMA((heads,)),
            pltpu.SemaphoreType.DMA((heads,)),
            pltpu.SemaphoreType.DMA((chips,)),
            pltpu.SemaphoreType.DMA((chips,)),
            pltpu.SemaphoreType.DMA((max(peers - 1, 1), chips)),
            pltpu.SemaphoreType.DMA((max(peers - 1, 1), chips)),
        ],
        compiler_params=pltpu.CompilerParams(
            collective_id=0, has_side_effects=True, vmem_limit_bytes=60 * 1024 * 1024
        ),
        name="gla_project",
    )
    outs = [
        call(queries[n], keys[n], values[n], gate_rate[n], segment_ids[n:n + 1], decay_exps, out_weight)
        for n in range(groups)
    ]
    return jnp.stack(outs)


def solution(mesh):
    in_specs = (
        P("batch", "seq", None),
        P("batch", "seq", None),
        P("batch", "seq", None),
        P("batch", "seq", None),
        P("batch", "seq"),
        P(),
        P("batch", None),
    )
    body = functools.partial(local, chip_grid(mesh), mesh.shape["seq"])
    return jax.shard_map(
        body, mesh=mesh, in_specs=in_specs, out_specs=P("batch", "seq", None), check_vma=False
    )
```

```python
import functools
import math

import jax
import jax.numpy as jnp
from jax import lax
from jax.experimental import pallas as pl
from jax.experimental.pallas import tpu as pltpu
from jax.sharding import PartitionSpec as P

MESH = pl.DeviceIdType.MESH
CHUNK = 256
TILE = 512


def chip_grid(mesh):
    count = mesh.shape["batch"]
    try:
        axis = mesh.axis_names.index("batch")
        line = mesh.devices.swapaxes(0, axis).reshape(count, -1)[:, 0]
        coords = [tuple(device.coords) for device in line]
        sizes = [len({c[i] for c in coords}) for i in (2, 1, 0)]
        lows = [min(c[i] for c in coords) for i in (2, 1, 0)]
        for index, c in enumerate(coords):
            z, y, x = (c[2] - lows[0], c[1] - lows[1], c[0] - lows[2])
            if (z * sizes[1] + y) * sizes[2] + x != index:
                return (count, 1, 1)
        return tuple(sizes)
    except Exception:
        return (count, 1, 1)


def split(x):
    high = x.astype(jnp.bfloat16)
    return high, (x - high.astype(jnp.float32)).astype(jnp.bfloat16)


def mm(a, b):
    return lax.dot_general(a, b, (((1,), (0,)), ((), ())), preferred_element_type=jnp.float32)


def mm_t(a, b):
    return lax.dot_general(a, b, (((1,), (1,)), ((), ())), preferred_element_type=jnp.float32)


def t_mm(a, b):
    return lax.dot_general(a, b, (((0,), (0,)), ((), ())), preferred_element_type=jnp.float32)


def kernel(
    grid, peers, heads, chunk,
    q_hbm, k_hbm, v_hbm, g_hbm, seg_ref, exps_ref, w_hbm,
    out_ref,
    q_ref, k_ref, v_ref, g_ref, w_ref, hidden, acc, seg_in, state_in, state_out,
    load_sem, seg_sem, state_send, state_recv, send_sem, recv_sem, climb_sem, msend, mrecv,
):
    Z, Y, X = grid
    s = lax.axis_index("seq")
    me = lax.axis_index("batch")
    length, keys = q_ref.shape
    key_width = keys // heads
    value_width = v_ref.shape[1] // heads
    rows = w_hbm.shape[0]
    columns = w_ref.shape[1]
    part = columns // peers
    plane_rows = rows * X * Y
    a = me // (X * Y)
    swap = X == Y
    nb, nc = X, Y

    def strides(core):
        if not swap:
            return 1, X
        even = lax.rem(core, 2) == 0
        return jnp.where(even, 1, X), jnp.where(even, X, 1)

    def chip_at(core, plane, db, dc):
        sb, sc = strides(core)
        b = lax.rem(me // sb, nb)
        c = lax.rem(me // sc, nc)
        return (
            plane * (X * Y)
            + lax.rem(b - db + nb, nb) * sb
            + lax.rem(c - dc + nc, nc) * sc
        )

    near = jnp.minimum(a, Z - 1 - a)

    def plane_at(g):
        side = jnp.where(lax.rem(g, 2) == 1, -1, 1)
        rest = jnp.where(a < Z - 1 - a, g, Z - 1 - g)
        return jnp.where(g <= 2 * near, a + (g + 1) // 2 * side, rest)

    def label(plane, db, dc):
        return (plane * nb + db) * nc + dc

    def block(core, chip):
        return w_ref.at[
            pl.ds(pl.multiple_of(chip * rows, rows), rows),
            pl.ds(pl.multiple_of(core * part, part), part),
        ]

    def relay(held, step):
        here = block(s, chip_at(s, *held))
        target = chip_at(s, a, -step[0], -step[1])
        index = label(held[0], held[1] + step[0], held[2] + step[1])
        return pltpu.make_async_remote_copy(
            src_ref=here, dst_ref=here, send_sem=send_sem.at[index], recv_sem=recv_sem.at[index],
            device_id={"batch": target}, device_id_type=MESH,
        )

    def climb(plane, way):
        here = block(s, chip_at(s, plane, 0, 0))
        target = me + (X * Y if way else -X * Y)
        return pltpu.make_async_remote_copy(
            src_ref=here, dst_ref=here, send_sem=climb_sem.at[way, plane],
            recv_sem=recv_sem.at[label(plane, 0, 0)],
            device_id={"batch": target}, device_id_type=MESH,
        )

    def arrival(plane, db, dc):
        here = block(s, chip_at(s, plane, db, dc))
        index = label(plane, db, dc)
        other = lax.rem(me + 1, X * Y * Z)
        return pltpu.make_async_remote_copy(
            src_ref=here, dst_ref=here, send_sem=send_sem.at[index], recv_sem=recv_sem.at[index],
            device_id={"batch": other}, device_id_type=MESH,
        )

    def mirror(plane, db, dc, ds, core):
        here = block(core, chip_at(core, plane, db, dc))
        index = label(plane, db, dc)
        return pltpu.make_async_remote_copy(
            src_ref=here, dst_ref=here,
            send_sem=msend.at[ds - 1, index], recv_sem=mrecv.at[ds - 1, index],
            device_id={"seq": lax.rem(s + ds, peers)}, device_id_type=MESH,
        )

    def share(plane, db, dc):
        for ds in range(1, peers):
            mirror(plane, db, dc, ds, s).start()

    def forward_plane(plane):
        for db in range(1, nb):
            relay((plane, 0, 0), (db, 0)).start()
        for dc in range(1, nc):
            relay((plane, 0, 0), (0, dc)).start()

    def middle(g):
        @pl.when(g < Z)
        def _():
            plane = plane_at(g)
            for db in range(1, nb):
                arrival(plane, db, 0).wait_recv()
                for dc in range(1, nc):
                    relay((plane, db, 0), (0, dc)).start()
                share(plane, db, 0)

    def enter(g):
        @pl.when(g < Z)
        def _():
            plane = plane_at(g)
            arrival(plane, 0, 0).wait_recv()

            @pl.when(jnp.logical_and(plane < a, a < Z - 1))
            def _():
                climb(plane, 1).start()

            @pl.when(jnp.logical_and(plane > a, a > 0))
            def _():
                climb(plane, 0).start()

            forward_plane(plane)
            share(plane, 0, 0)

    def tail(g):
        @pl.when(g < Z)
        def _():
            plane = plane_at(g)
            for dc in range(1, nc):
                for db in range(nb):
                    arrival(plane, db, dc).wait_recv()
                    share(plane, db, dc)

    def mirrored(g):
        plane = plane_at(g)
        for ds in range(1, peers):
            core = lax.rem(s - ds + peers, peers)
            for db in range(nb):
                for dc in range(nc):
                    def wait():
                        mirror(plane, db, dc, ds, core).wait_recv()
                    if db or dc:
                        wait()
                    else:
                        pl.when(g > 0)(wait)

    loads = [
        pltpu.make_async_copy(
            w_hbm, w_ref.at[pl.ds(pl.multiple_of(me * rows, rows), rows), :], load_sem.at[0]
        ),
        pltpu.make_async_copy(g_hbm, g_ref, load_sem.at[1]),
        pltpu.make_async_copy(k_hbm, k_ref, load_sem.at[2]),
        pltpu.make_async_copy(q_hbm, q_ref, load_sem.at[3]),
        pltpu.make_async_copy(v_hbm, v_ref, load_sem.at[4]),
    ]
    for load in loads:
        load.start()

    barrier = pltpu.get_barrier_semaphore()
    friends = [{"batch": chip_at(s, a, d, 0)} for d in range(1, nb)]
    friends += [{"batch": chip_at(s, a, 0, d)} for d in range(1, nc)]
    friends += [{"seq": lax.rem(s + d, peers)} for d in range(1, peers)]
    for friend in friends:
        pl.semaphore_signal(barrier, inc=1, device_id=friend, device_id_type=MESH)

    @pl.when(a < Z - 1)
    def _():
        pl.semaphore_signal(barrier, inc=1, device_id={"batch": me + X * Y}, device_id_type=MESH)

    @pl.when(a > 0)
    def _():
        pl.semaphore_signal(barrier, inc=1, device_id={"batch": me - X * Y}, device_id_type=MESH)

    above, below = jnp.where(a < Z - 1, 1, 0), jnp.where(a > 0, 1, 0)
    pl.semaphore_wait(barrier, len(friends) + above + below)

    loads[0].wait()

    @pl.when(a < Z - 1)
    def _():
        climb(a, 1).start()

    @pl.when(a > 0)
    def _():
        climb(a, 0).start()

    forward_plane(a)

    def next_core():
        return {"seq": lax.rem(s + 1, peers)}

    seg_copy = pltpu.make_async_remote_copy(
        src_ref=seg_ref, dst_ref=seg_in, send_sem=seg_sem.at[0], recv_sem=seg_sem.at[1],
        device_id=next_core(), device_id_type=MESH,
    )

    def state_copy(h):
        return pltpu.make_async_remote_copy(
            src_ref=state_out.at[h], dst_ref=state_in.at[h],
            send_sem=state_send.at[h], recv_sem=state_recv.at[h],
            device_id=next_core(), device_id_type=MESH,
        )

    @pl.when(s < peers - 1)
    def _():
        seg_copy.start()

    @pl.when(s == 0)
    def _():
        state_in[...] = jnp.zeros_like(state_in)
        seg_in[...] = jnp.full(seg_in.shape, -1, jnp.int32)

    for load in loads[1:]:
        load.wait()

    @pl.when(s > 0)
    def _():
        seg_copy.wait_recv()

    order_t = lax.broadcasted_iota(jnp.int32, (chunk, chunk), 0)
    order_s = lax.broadcasted_iota(jnp.int32, (chunk, chunk), 1)
    causal = order_t >= order_s
    triangle = jnp.where(causal, 1.0, 0.0).astype(jnp.bfloat16)
    seg_row = seg_ref[...].astype(jnp.float32)
    before = seg_in[...].astype(jnp.float32)[:, length - 1:]
    seg_wide = jnp.broadcast_to(seg_row, (128, length)).T

    def first():
        middle(0)
        enter(1)

    def second():
        enter(2)
        middle(1)

    def third():
        enter(3)
        tail(0)

    events = [first, second, third]
    early = min(len(events), heads - 1)

    def head(h, _):
        turn = h - jnp.where(s == 0, 1, 0)
        for number, event in enumerate(events[:early]):
            pl.when(turn == number)(event)

        exponent = jnp.full((1, key_width), exps_ref[h], jnp.int32).astype(jnp.float32)
        scale = jnp.exp2(-exponent) * (-1.0 / 16.0)

        @pl.when(s > 0)
        def _():
            state_copy(h).wait_recv()

        state = state_in[h]
        previous = before
        key_cols = pl.ds(pl.multiple_of(h * key_width, key_width), key_width)
        value_cols = pl.ds(pl.multiple_of(h * value_width, value_width), value_width)
        for i in range(length // chunk):
            now = pl.ds(i * chunk, chunk)
            log = mm(triangle, g_ref[now, key_cols]) * scale
            fall = jnp.exp(log)
            raised_q = q_ref[now, key_cols].astype(jnp.float32) * (fall * (1.0 / math.sqrt(key_width)))
            raised_k = k_ref[now, key_cols].astype(jnp.float32) * jnp.exp(-log)
            value = v_ref[now, value_cols]
            q_hi, q_lo = split(raised_q)
            k_hi, k_lo = split(raised_k)
            row = seg_row[:, i * chunk:(i + 1) * chunk]
            column = seg_wide[i * chunk:(i + 1) * chunk, :1]
            scores = mm_t(q_hi, k_hi) + mm_t(q_hi, k_lo) + mm_t(q_lo, k_hi)
            scores = jnp.where(jnp.logical_and(causal, column == row), scores, 0.0)
            p_hi, p_lo = split(scores)
            s_hi, s_lo = split(state)
            carried = mm_t(q_hi, s_hi) + mm_t(q_hi, s_lo) + mm_t(q_lo, s_hi)
            mixed = mm(p_hi, value) + mm(p_lo, value)
            mixed = mixed + jnp.where(column == previous, carried, 0.0)
            power = jnp.mean(mixed * mixed, axis=-1, keepdims=True)
            hidden[now, value_cols] = (mixed * lax.rsqrt(power + 1.0)).astype(jnp.bfloat16)
            final = fall[chunk - 1:, :]
            last = row[:, chunk - 1:]
            weighted = jnp.where(column == last, raised_k * final, 0.0)
            w_hi, w_lo = split(weighted)
            kept = jnp.where(last == previous, state * final, 0.0)
            state = kept + t_mm(value, w_hi) + t_mm(value, w_lo)
            previous = last

        @pl.when(s < peers - 1)
        def _():
            state_out[h] = state
            state_copy(h).start()

        return 0

    lax.fori_loop(0, heads, head, 0)
    for event in events[early:]:
        event()

    def plane_start(g):
        return pl.multiple_of(plane_at(g) * plane_rows, plane_rows)

    def project(g):
        start = plane_start(g)
        left = hidden[:, pl.ds(start, plane_rows)]
        for tile in range(columns // TILE):
            cols = pl.ds(tile * TILE, TILE)
            product = mm(left, w_ref[pl.ds(start, plane_rows), cols])

            @pl.when(g == 0)
            def _():
                acc[:, cols] = product

            @pl.when(g > 0)
            def _():
                acc[:, cols] += product

    def step(g, _):
        middle(g + 2)
        enter(g + 4)
        mirrored(g)
        project(g)
        tail(g + 1)
        return 0

    lax.fori_loop(0, Z - 1, step, 0)
    mirrored(Z - 1)
    start = plane_start(Z - 1)
    left = hidden[:, pl.ds(start, plane_rows)]
    for tile in range(columns // TILE):
        cols = pl.ds(tile * TILE, TILE)
        product = mm(left, w_ref[pl.ds(start, plane_rows), cols])
        total = acc[:, cols] + product if Z > 1 else product
        out_ref[:, cols] = total.astype(jnp.bfloat16)

    @pl.when(s < peers - 1)
    def _():
        seg_copy.wait_send()

        def sent(h, _):
            state_copy(h).wait_send()
            return 0

        lax.fori_loop(0, heads, sent, 0)

    def sent_plane(plane, _):
        for db in range(nb):
            for dc in range(nc):
                if db or dc:
                    arrival(plane, db, dc).wait_send()

                def wait():
                    for ds in range(1, peers):
                        mirror(plane, db, dc, ds, s).wait_send()

                if db or dc:
                    wait()
                else:
                    pl.when(plane != a)(wait)

        @pl.when(jnp.logical_and(plane <= a, a < Z - 1))
        def _():
            climb(plane, 1).wait_send()

        @pl.when(jnp.logical_and(plane >= a, a > 0))
        def _():
            climb(plane, 0).wait_send()

        return 0

    lax.fori_loop(0, Z, sent_plane, 0)


def local(grid, peers, queries, keys, values, gate_rate, segment_ids, decay_exps, out_weight):
    groups, length, key_features = queries.shape
    heads = decay_exps.shape[0]
    features = values.shape[2]
    columns = out_weight.shape[1]
    chips = grid[0] * grid[1] * grid[2]
    chunk = min(CHUNK, length)
    kw, vw = key_features // heads, features // heads
    bf16, f32 = jnp.bfloat16, jnp.float32
    anywhere = pl.BlockSpec(memory_space=pl.ANY)
    call = pl.pallas_call(
        functools.partial(kernel, grid, peers, heads, chunk),
        out_shape=pltpu.VMEM((length, columns), bf16),
        in_specs=[anywhere] * 4
        + [pl.BlockSpec(memory_space=pltpu.VMEM), pl.BlockSpec(memory_space=pltpu.SMEM), anywhere],
        out_specs=pl.BlockSpec(memory_space=pltpu.VMEM),
        scratch_shapes=[
            pltpu.VMEM((length, key_features), bf16),
            pltpu.VMEM((length, key_features), bf16),
            pltpu.VMEM((length, features), bf16),
            pltpu.VMEM((length, key_features), bf16),
            pltpu.VMEM((features, columns), bf16),
            pltpu.VMEM((length, features), bf16),
            pltpu.VMEM((length, columns), f32),
            pltpu.VMEM((1, length), jnp.int32),
            pltpu.VMEM((heads, vw, kw), f32),
            pltpu.VMEM((heads, vw, kw), f32),
            pltpu.SemaphoreType.DMA((5,)),
            pltpu.SemaphoreType.DMA((2,)),
            pltpu.SemaphoreType.DMA((heads,)),
            pltpu.SemaphoreType.DMA((heads,)),
            pltpu.SemaphoreType.DMA((chips,)),
            pltpu.SemaphoreType.DMA((chips,)),
            pltpu.SemaphoreType.DMA((2, grid[0])),
            pltpu.SemaphoreType.DMA((max(peers - 1, 1), chips)),
            pltpu.SemaphoreType.DMA((max(peers - 1, 1), chips)),
        ],
        compiler_params=pltpu.CompilerParams(
            collective_id=0, has_side_effects=True, vmem_limit_bytes=61 * 1024 * 1024
        ),
        name="gla_project",
    )
    outs = [
        call(queries[n], keys[n], values[n], gate_rate[n], segment_ids[n:n + 1], decay_exps, out_weight)
        for n in range(groups)
    ]
    return jnp.stack(outs)


def solution(mesh):
    in_specs = (
        P("batch", "seq", None),
        P("batch", "seq", None),
        P("batch", "seq", None),
        P("batch", "seq", None),
        P("batch", "seq"),
        P(),
        P("batch", None),
    )
    body = functools.partial(local, chip_grid(mesh), mesh.shape["seq"])
    return jax.shard_map(
        body, mesh=mesh, in_specs=in_specs, out_specs=P("batch", "seq", None), check_vma=False
    )
```
